32 devices in a mesh: group: 2 (over y), plane: 4 (over z), planey: 2 (over x), ens: 2 (over core).
Axes of the slice: x: 2, y: 2, z: 4, core: 2. Of those that a mesh axis runs over, the one named last changes fastest.
Arguments:
- u_prior: float32 [8, 2, 10, 64, 256], P(('group', 'ens'), None, None, 'plane', 'planey'), parts along dimension 0, may hold values from -6 to 6
- friction_rows: int32 [8], P(('group', 'ens')), parts along dimension 0, may hold values from 0 to 15
- friction_table: float32 [32, 64, 256], P('group', 'plane', 'planey'), parts along dimension 0, may hold values from 0.3 to 3
- bed_fixed: int32 [64, 256], P('plane', 'planey'), may hold values from -536870912 to 536870911
- ice_mask: int32 [64, 256], P('plane', 'planey'), may hold values 0 or 1
Outputs:
- mean_velocity: float32 [4, 10, 64, 256], P('group', None, 'plane', 'planey'), parts along dimension 0
The draws below stay inside these ranges and needn't reach their ends.
There are 2 independent parts, one for each index of `group`. The reference program is written for one: setup_inputs(seed, part) draws one part's arguments, and reference() takes and returns one part's arrays. A program takes and returns all parts, laid end to end along the dimension named above; an argument that names none is the same for every part. Nothing has to cross between parts.
Inputs may be any that keep to these rules, and one draw needn't show every extreme that they name: `friction_rows`: each sample names one row of the friction table.
All inputs are finite; a program needn't handle non-finite values. No bound on the sum of `ice_mask` on one device may be relied on, other than what follows from the above.
Results may differ from the reference program's by a relative error of at most 0.0003.
Values sent between devices are 32-bit elements; how exact they have to be, the bound alone decides.
A program may use at most 64 MiB of HBM per device.

```python
import math
import jax
import jax.numpy as jnp
from jax import lax

NZ = 10
ITERS = 2
LEVELS = 16
SAMPLES = 4
NX = 64
NY = 256


def with_ends(drawn, rng, least, largest):
    spot = [jax.random.randint(jax.random.fold_in(rng, axis), (), 0, length) for axis, length in enumerate(drawn.shape)]
    main_axis = drawn.shape.index(max(drawn.shape))
    next_to = spot[:main_axis] + [(spot[main_axis] + 1) % drawn.shape[main_axis]] + spot[main_axis + 1:]
    return drawn.at[tuple(spot)].set(least).at[tuple(next_to)].set(largest)


def shard_levels(stream_key, dims, shards, smallest, top_value):
    factor_of, own = 1.0, jax.random.fold_in(stream_key, 6)
    for axis_at, blocks in shards:
        draws = jnp.exp(jax.random.uniform(jax.random.fold_in(own, axis_at), (blocks,), jnp.float32, smallest / len(shards), top_value / len(shards)))
        factor_of = factor_of * jnp.repeat(draws, dims[axis_at] // blocks).reshape([-1 if axis == axis_at else 1 for axis in range(len(dims))])
    return factor_of


def scatter_about(stream_key, shape, width, bound, split=(), kind=jnp.bfloat16):
    values = jax.random.normal(stream_key, shape, jnp.float32) * width
    if len(split) > 0:
        values = shard_levels(stream_key, shape, split, -0.22, 0.18) * values
    return jnp.clip(values, min=-bound, max=bound).astype(kind)


def setup_inputs(seed: int = 0, part: int = 0) -> dict:
    keys = jax.random.split(jax.random.key(seed), 6)
    own_keys = jax.random.split(jax.random.fold_in(keys[5], part), 6)
    return {
        "u_prior": scatter_about(own_keys[0], (SAMPLES, 2, NZ, NX, NY), 1.0, 6.0, ((0, 2), (3, 4), (4, 2)), jnp.float32),
        "friction_rows": with_ends(jax.random.randint(own_keys[1], (SAMPLES,), 0, LEVELS), jax.random.fold_in(own_keys[1], 1), 0, LEVELS - 1).astype(jnp.int32),
        "friction_table": jnp.clip(jnp.exp(math.log(3.0) - 2.3025851 * jax.random.uniform(own_keys[2], (LEVELS, NX, NY), jnp.float32) ** shard_levels(own_keys[2], (LEVELS, NX, NY), ((1, 4), (2, 2)), -0.2, 0.2)), 0.3, 3.0),
        "bed_fixed": with_ends(jax.random.randint(keys[3], (NX, NY), -536870912, 536870912), jax.random.fold_in(keys[3], 1), -536870912, 536870911).astype(jnp.int32),
        "ice_mask": with_ends((jax.random.randint(keys[4], (NX, NY), 0, 8) < 7).astype(jnp.int32), jax.random.fold_in(keys[4], 1), 0, 1),
    }


bed_unit = 2.0 ** -29
factor_u = (2.0, 1.0, 0.5)
factor_v = (2.0, 0.5, 1.0)


def coefficient(offset):
    nonzero = len([entry for entry in offset if entry != 0])
    weight_u = 0.25 ** (nonzero - 1)
    weight_v = weight_u
    for dimension in range(3):
        if offset[dimension] != 0:
            weight_u = weight_u * factor_u[dimension]
            weight_v = weight_v * factor_v[dimension]
    return jnp.array([weight_u, weight_v], jnp.float32).reshape(2, 1, 1, 1)


def neighbour_sum(padded):
    layers = padded.shape[-3] - 2
    span_x = padded.shape[-2] - 2
    span_y = padded.shape[-1] - 2
    summed = None
    for step_z in (-1, 0, 1):
        for step_x in (-1, 0, 1):
            for step_y in (-1, 0, 1):
                if step_z == 0 and step_x == 0 and step_y == 0:
                    continue
                window = padded[..., 1 + step_z:1 + step_z + layers, 1 + step_x:1 + step_x + span_x, 1 + step_y:1 + step_y + span_y]
                addend = coefficient((step_z, step_x, step_y)) * window
                summed = addend if summed is None else summed + addend
    return summed


def strain_roots(extended):
    padded = jnp.pad(extended, [(0, 0)] * (extended.ndim - 3) + [(1, 1), (0, 0), (0, 0)])
    along_x = (padded[..., 1:-1, 2:, 1:-1] - padded[..., 1:-1, :-2, 1:-1]) * 0.5
    along_y = (padded[..., 1:-1, 1:-1, 2:] - padded[..., 1:-1, 1:-1, :-2]) * 0.5
    along_z = (padded[..., 2:, 1:-1, 1:-1] - padded[..., :-2, 1:-1, 1:-1]) * 0.5
    stretch_x = along_x[..., 0, :, :, :]
    stretch_y = along_y[..., 1, :, :, :]
    shear_one = along_y[..., 0, :, :, :]
    shear_two = along_x[..., 1, :, :, :]
    vertical_u = along_z[..., 0, :, :, :]
    vertical_v = along_z[..., 1, :, :, :]
    shear = shear_one + shear_two
    strain = stretch_x * stretch_x + stretch_y * stretch_y + stretch_x * stretch_y + 0.25 * shear * shear + 0.25 * (vertical_u * vertical_u + vertical_v * vertical_v)
    return jnp.power(strain + 0.1, -1.0 / 6.0)[..., None, :, :, :]


def reference(u_prior, friction_rows, friction_table, bed_fixed, ice_mask):
    cover = ice_mask.astype(jnp.float32)
    bed = bed_fixed.astype(jnp.float32) * bed_unit
    bed_pad = jnp.pad(bed, 1)
    slope_x = (bed_pad[2:, 1:-1] - bed_pad[:-2, 1:-1]) * 0.5
    slope_y = (bed_pad[1:-1, 2:] - bed_pad[1:-1, :-2]) * 0.5
    thickness = 1.0 + 2.0 * jnp.arange(NX, dtype=jnp.float32)[:, None] / (NX - 1)
    force = jnp.stack([-(cover * thickness * slope_x), -(cover * thickness * slope_y)])[:, None, :, :]
    bottom = (jnp.arange(NZ, dtype=jnp.int32) == 0).astype(jnp.float32)[:, None, None]
    levels = jnp.arange(LEVELS, dtype=jnp.int32)

    def solve(summed, inputs):
        prior, table_row = inputs
        extended = jnp.pad(prior, ((0, 0), (0, 0), (1, 1), (1, 1)))
        roots = cover * strain_roots(extended)
        across = neighbour_sum(jnp.pad(roots, ((0, 0), (1, 1), (1, 1), (1, 1))))
        chosen = (levels == table_row).astype(jnp.float32)
        friction = jnp.sum(chosen[:, None, None] * friction_table, axis=0)
        diag = cover * friction * bottom + (1.0 - cover)

        def operate(field):
            product = roots * field
            nearby = neighbour_sum(jnp.pad(product, ((0, 0), (1, 1), (1, 1), (1, 1))))
            return roots * (across * field - nearby) + diag * field

        solution = prior * cover
        residual = force - operate(solution)
        direction = residual
        norm_now = jnp.sum(residual * residual)
        for step in range(ITERS):
            image = operate(direction)
            alpha = norm_now / jnp.sum(direction * image)
            solution = solution + alpha * direction
            if step + 1 < ITERS:
                residual = residual - alpha * image
                norm_next = jnp.sum(residual * residual)
                direction = residual + (norm_next / norm_now) * direction
                norm_now = norm_next
        return summed + solution, None

    start = jnp.zeros((2, NZ, NX, NY), jnp.float32)
    summed = lax.scan(solve, start, (u_prior, friction_rows))[0]
    return summed / SAMPLES
```

```python
import functools
import jax
import jax.numpy as jnp
from jax import lax
from jax.experimental import pallas as pl
from jax.experimental.pallas import tpu as pltpu
from jax.sharding import PartitionSpec as P

bed_unit = 2.0 ** (-29)
HALO = 4
SLOTS = 16
STEP_I = (0.25, 0.125)
STEP_J = (0.125, 0.25)


def iota(shape, dim):
    return lax.broadcasted_iota(jnp.int32, shape, dim)


def shift_i(x, step):
    return pltpu.roll(x, (-step) % x.shape[-2], x.ndim - 2)


def shift_j(x, step):
    rolled = pltpu.roll(x, (-step) % x.shape[-1], x.ndim - 1)
    swapped = jnp.concatenate([rolled[1:2], rolled[0:1]], axis=0)
    lane = iota(x.shape, x.ndim - 1)
    edge = 0 if step < 0 else x.shape[-1] - 1
    return jnp.where(lane == edge, swapped, rolled)


def spread_ij(x, c):
    x = x + STEP_I[c] * (shift_i(x, 1) + shift_i(x, -1))
    return x + STEP_J[c] * (shift_j(x, 1) + shift_j(x, -1))


def spread_z(ref, index, z):
    return ref[index + (z + 1,)] + 0.5 * (ref[index + (z,)] + ref[index + (z + 2,)])


def kernel(sizes, rows_ref, u_hbm, table_hbm, bed_hbm, mask_hbm, out_ref,
           u_v, table_v, bed_v, mask_v,
           up_s, down_s, side_s, corner_s,
           below_r, above_r, side_r, corner_r, hx,
           ext, roots, tr, pa, pb, r_ext, a_ext, force,
           r_core, a_core, w_core, r_peer, a_peer, w_peer,
           gram_s, gram_r,
           in_sem, halo_send, halo_recv, peer_send, peer_recv, gram_send, gram_recv):
    np_, nq, ne = sizes
    members, _, layers, rows, cols = u_v.shape
    ring = rows + 2 * HALO
    ix, iy, ie = lax.axis_index("plane"), lax.axis_index("planey"), lax.axis_index("ens")

    loads = [
        pltpu.make_async_copy(src, dst, in_sem.at[i])
        for i, (src, dst) in enumerate(
            ((u_hbm, u_v), (table_hbm, table_v), (bed_hbm, bed_v), (mask_hbm, mask_v))
        )
    ]
    for load in loads:
        load.start()

    def group_target(d):
        de, rest = d // (np_ * nq), d % (np_ * nq)
        return {
            "plane": lax.rem(ix + rest // nq, np_),
            "planey": lax.rem(iy + rest % nq, nq),
            "ens": lax.rem(ie + de, ne),
        }

    total = np_ * nq * ne

    def each_peer(fn):
        if total <= 32:
            for d in range(1, total):
                fn(d)
        else:
            def step(d, carry):
                fn(d)
                return carry
            lax.fori_loop(1, total, step, 0)

    barrier = pltpu.get_barrier_semaphore()
    each_peer(lambda d: pl.semaphore_signal(
        barrier, inc=1, device_id=group_target(d), device_id_type=pl.DeviceIdType.MESH))

    flows = []
    for i, (dx, dy, src, dst) in enumerate((
        (-1, 0, up_s, below_r),
        (1, 0, down_s, above_r),
        (0, -1, side_s, side_r.at[1]),
        (0, 1, side_s, side_r.at[0]),
        (-1, -1, corner_s, corner_r.at[0, 1]),
        (-1, 1, corner_s, corner_r.at[0, 0]),
        (1, -1, corner_s, corner_r.at[1, 1]),
        (1, 1, corner_s, corner_r.at[1, 0]),
    )):
        tx, ty = ix + dx, iy + dy
        sx, sy = ix - dx, iy - dy
        to_ok = (tx >= 0) & (tx < np_) & (ty >= 0) & (ty < nq)
        from_ok = (sx >= 0) & (sx < np_) & (sy >= 0) & (sy < nq)
        copy = pltpu.make_async_remote_copy(
            src_ref=src, dst_ref=dst, send_sem=halo_send.at[i], recv_sem=halo_recv.at[i],
            device_id={"plane": jnp.clip(tx, 0, np_ - 1), "planey": jnp.clip(ty, 0, nq - 1)},
            device_id_type=pl.DeviceIdType.MESH)
        flows.append((copy, to_ok, from_ok, dst))

    for load in loads:
        load.wait()

    planes = [(lambda m=m, c=c, z=z: u_v[m, c, z])
              for m in range(members) for z in range(layers) for c in range(2)]
    first_extra = len(planes)
    planes.append(lambda: bed_v[...].astype(jnp.float32) * bed_unit)
    planes.append(lambda: mask_v[...].astype(jnp.float32))
    for m in range(members):
        planes.append(lambda m=m: table_v[rows_ref[m]])
    if len(planes) % 2:
        planes.append(planes[-1])
    groups = side_s.shape[0]

    low8 = iota((8, cols), 0) < 4
    lane_x = iota((rows, cols), 1)
    for g in range(groups):
        packed = jnp.zeros((rows, cols), jnp.float32)
        for k in range(SLOTS):
            p = g * SLOTS + k
            if p >= len(planes):
                continue
            rolled = pltpu.roll(planes[p](), (8 * k + 4) % cols, 1)
            packed = jnp.where((lane_x // 8) == k, rolled, packed)
        side_s[g] = packed
        corner_s[g] = jnp.where(low8, packed[0:8], packed[rows - 8:rows])

    def ends(value):
        return jnp.where(low8, value[0:8], value[rows - 8:rows])

    for i in range(len(planes) // 2):
        first = ends(planes[2 * i]())
        turned = pltpu.roll(ends(planes[2 * i + 1]()), 4, 0)
        up_s[i] = jnp.where(low8, first, turned)
        down_s[i] = jnp.where(low8, turned, first)

    pl.semaphore_wait(barrier, total - 1)
    for copy, to_ok, from_ok, dst in flows:
        pl.when(to_ok)(copy.start)

    for copy, to_ok, from_ok, dst in flows:
        @pl.when(jnp.logical_not(from_ok))
        def _(dst=dst):
            dst[...] = jnp.zeros(dst.shape, jnp.float32)
    zero = jnp.zeros((2, ring, cols), jnp.float32)
    for m in range(members):
        for end in (0, layers + 1):
            roots[m, end] = zero
            for c in range(2):
                ext[m, c, end] = zero
                pa[m, c, end] = zero
                pb[m, c, end] = zero
    cover_core = mask_v[...].astype(jnp.float32)
    for c in range(2):
        for z in range(layers):
            summed = u_v[0, c, z]
            for m in range(1, members):
                summed = summed + u_v[m, c, z]
            w_core[c, z] = cover_core * summed

    for copy, to_ok, from_ok, dst in flows:
        pl.when(from_ok)(copy.wait_recv)

    lane_h = iota((rows, cols), 1)
    lane_8 = iota((8, cols), 1)
    for g in range(groups):
        hx[g, 0:rows] = jnp.where(lane_h % 8 < 4, side_r[0, g], side_r[1, g])
        left = jnp.where(low8, corner_r[0, 0, g], corner_r[1, 0, g])
        right = jnp.where(low8, corner_r[0, 1, g], corner_r[1, 1, g])
        hx[g, rows:ring] = jnp.where(lane_8 % 8 < 4, left, right)

    def tail(p):
        i = p // 2
        if p % 2 == 0:
            return jnp.where(low8, below_r[i], above_r[i])
        return pltpu.roll(jnp.where(low8, above_r[i], below_r[i]), 4, 0)

    def extended(p):
        core = jnp.concatenate([planes[p](), tail(p)], axis=0)
        k = p % SLOTS
        halo = pltpu.roll(hx[p // SLOTS], (-(8 * k + 4)) % cols, 1)
        return jnp.stack([core, halo])

    p = 0
    for m in range(members):
        for z in range(layers):
            for c in range(2):
                ext[m, c, z + 1] = extended(p)
                p += 1
    bed = extended(first_extra)
    cover = extended(first_extra + 1)
    row = iota((2, ring, cols), 1)
    position = (ix * rows + jnp.where(row < rows + HALO, row, row - ring)).astype(jnp.float32)
    thickness = 1.0 + 2.0 * position / (np_ * rows - 1)
    slope_x = (shift_i(bed, 1) - shift_i(bed, -1)) * 0.5
    slope_y = (shift_j(bed, 1) - shift_j(bed, -1)) * 0.5
    force[0] = -(cover * thickness * slope_x)
    force[1] = -(cover * thickness * slope_y)
    force[2] = cover
    for m in range(members):
        force[3 + m] = cover * extended(first_extra + 2 + m)

    def roots_step(z, carry):
        cover = force[2]
        for m in range(members):
            u, v = ext[m, 0, z + 1], ext[m, 1, z + 1]
            u_i = (shift_i(u, 1) - shift_i(u, -1)) * 0.5
            v_j = (shift_j(v, 1) - shift_j(v, -1)) * 0.5
            shear = ((shift_j(u, 1) - shift_j(u, -1)) + (shift_i(v, 1) - shift_i(v, -1))) * 0.5
            u_z = (ext[m, 0, z + 2] - ext[m, 0, z]) * 0.5
            v_z = (ext[m, 1, z + 2] - ext[m, 1, z]) * 0.5
            strain = (u_i * u_i + v_j * v_j + u_i * v_j + 0.25 * shear * shear
                      + 0.25 * (u_z * u_z + v_z * v_z))
            root = cover * jnp.exp(jnp.log(strain + 0.1) * (-1.0 / 6.0))
            roots[m, z + 1] = root
            pa[m, 0, z + 1] = root * u
            pa[m, 1, z + 1] = root * v
        return carry

    lax.fori_loop(0, layers, roots_step, 0)

    def image(m, c, z, field, p_ref):
        across = tr[m, c, z]
        bottom = jnp.where(z == 0, 1.0, 0.0).astype(jnp.float32)
        diag = force[3 + m] * bottom + (1.0 - force[2])
        spread = spread_ij(spread_z(p_ref, (m, c), z), c)
        return 4.0 * roots[m, z + 1] * (across * field - spread) + diag * field

    zero_core = jnp.zeros((rows, cols), jnp.float32)

    def residual_step(z, carry):
        carry = list(carry)
        for m in range(members):
            near = spread_z(roots, (m,), z)
            for c in range(2):
                tr[m, c, z] = spread_ij(near, c)
                start = force[2] * ext[m, c, z + 1]
                r = force[c] - image(m, c, z, start, pa)
                r_ext[m, c, z] = r
                pb[m, c, z + 1] = roots[m, z + 1] * r
                core = r[0, 0:rows]
                r_core[m, c, z] = core
                carry[m] = carry[m] + core * core
        return tuple(carry)

    rr = lax.fori_loop(0, layers, residual_step, (zero_core,) * members)

    peer = {"ens": lax.rem(ie + 1, ne)}

    def to_peer(i, src, dst):
        return pltpu.make_async_remote_copy(
            src_ref=src, dst_ref=dst, send_sem=peer_send.at[i], recv_sem=peer_recv.at[i],
            device_id=peer, device_id_type=pl.DeviceIdType.MESH)

    peer_flows = [to_peer(0, w_core, w_peer), to_peer(1, r_core, r_peer), to_peer(2, a_core, a_peer)]
    peer_flows[0].start()

    def image_step(z, carry):
        carry = list(carry)
        for m in range(members):
            for c in range(2):
                r = r_ext[m, c, z]
                a = image(m, c, z, r, pb)
                a_ext[m, c, z] = a
                pa[m, c, z + 1] = roots[m, z + 1] * a
                core = a[0, 0:rows]
                a_core[m, c, z] = core
                carry[2 * m] = carry[2 * m] + r[0, 0:rows] * core
                carry[2 * m + 1] = carry[2 * m + 1] + core * core
        return tuple(carry)

    ra_aa = lax.fori_loop(0, layers, image_step, (zero_core,) * (2 * members))
    peer_flows[1].start()

    def second_step(z, carry):
        carry = list(carry)
        for m in range(members):
            for c in range(2):
                a = a_ext[m, c, z]
                b = image(m, c, z, a, pa)
                carry[m] = carry[m] + a[0, 0:rows] * b[0, 0:rows]
        return tuple(carry)

    ab = lax.fori_loop(0, layers, second_step, (zero_core,) * members)
    peer_flows[2].start()

    lane_1 = iota((1, cols), 1)
    mine = jnp.zeros((1, cols), jnp.float32)
    for m in range(members):
        for q, acc in enumerate((rr[m], ra_aa[2 * m], ra_aa[2 * m + 1], ab[m])):
            value = jnp.sum(jnp.sum(acc, axis=0, keepdims=True), axis=1, keepdims=True)
            mine = jnp.where(lane_1 == 4 * m + q, value, mine)
    gram_s[0] = mine

    def gram_copy(d):
        return pltpu.make_async_remote_copy(
            src_ref=gram_s, dst_ref=gram_r.at[pl.ds(d, 1)],
            send_sem=gram_send, recv_sem=gram_recv,
            device_id=group_target(d), device_id_type=pl.DeviceIdType.MESH)

    each_peer(lambda d: gram_copy(d).start())
    everything = pltpu.make_async_remote_copy(
        src_ref=gram_r.at[pl.ds(1, total - 1)], dst_ref=gram_r.at[pl.ds(1, total - 1)],
        send_sem=gram_send, recv_sem=gram_recv,
        device_id=group_target(1), device_id_type=pl.DeviceIdType.MESH)
    everything.wait_recv()

    half = np_ * nq
    own = mine
    if half > 1:
        own = own + jnp.sum(gram_r[1:half], axis=0)
    sums = [own] + [jnp.sum(gram_r[half * e:half * (e + 1)], axis=0) for e in range(1, ne)]
    steps = []
    for e in range(ne):
        for m in range(members):
            g_rr, g_ra, g_aa, g_ab = [
                jnp.sum(jnp.where(lane_1 == 4 * m + q, sums[e], 0.0), axis=1, keepdims=True)
                for q in range(4)
            ]
            first = g_rr / g_ra
            following = g_rr - 2.0 * first * g_ra + first * first * g_aa
            growth = 1.0 + following / g_rr
            curve = (growth * growth * g_ra - 2.0 * growth * first * g_aa
                     + first * first * g_ab)
            second = following / curve
            share = 1.0 / (members * ne)
            steps.append(((first + second * growth) * share, second * first * share))

    for flow in peer_flows:
        flow.wait_recv()
    share = 1.0 / (members * ne)

    def final_step(z, carry):
        for c in range(2):
            value = share * (w_core[c, z] + w_peer[c, z])
            for m in range(members):
                value = value + steps[m][0] * r_core[m, c, z] - steps[m][1] * a_core[m, c, z]
                one, two = steps[members + m]
                value = value + one * r_peer[m, c, z] - two * a_peer[m, c, z]
            out_ref[c, z] = value
        return carry

    lax.fori_loop(0, layers, final_step, 0)

    for copy, to_ok, from_ok, dst in flows:
        pl.when(to_ok)(copy.wait_send)
    for flow in peer_flows:
        flow.wait_send()
    everything.wait_send()


def body(sizes, u_prior, friction_rows, friction_table, bed_fixed, ice_mask):
    members, _, layers, rows, cols = u_prior.shape
    levels = friction_table.shape[0]
    total = sizes[0] * sizes[1] * sizes[2]
    ring = rows + 2 * HALO
    planes = members * layers * 2 + 2 + members
    pairs = (planes + 1) // 2
    groups = (2 * pairs + SLOTS - 1) // SLOTS
    f32 = jnp.float32
    any_space = pl.BlockSpec(memory_space=pl.ANY)
    vmem = lambda *shape: pltpu.VMEM(shape, f32)
    core = (members, 2, layers, rows, cols)
    wide = (2, ring, cols)
    return pl.pallas_call(
        functools.partial(kernel, sizes),
        out_shape=jax.ShapeDtypeStruct((2, layers, rows, cols), f32),
        in_specs=[pl.BlockSpec(memory_space=pltpu.SMEM)] + [any_space] * 4,
        out_specs=pl.BlockSpec(memory_space=pltpu.VMEM),
        scratch_shapes=[
            vmem(*core), vmem(levels, rows, cols),
            pltpu.VMEM((rows, cols), jnp.int32), pltpu.VMEM((rows, cols), jnp.int32),
            vmem(pairs, 8, cols), vmem(pairs, 8, cols), vmem(groups, rows, cols), vmem(groups, 8, cols),
            vmem(pairs, 8, cols), vmem(pairs, 8, cols), vmem(2, groups, rows, cols),
            vmem(2, 2, groups, 8, cols), vmem(groups, ring, cols),
            vmem(members, 2, layers + 2, *wide), vmem(members, layers + 2, *wide),
            vmem(members, 2, layers, *wide),
            vmem(members, 2, layers + 2, *wide), vmem(members, 2, layers + 2, *wide),
            vmem(members, 2, layers, *wide), vmem(members, 2, layers, *wide),
            vmem(3 + members, *wide),
            vmem(*core), vmem(*core), vmem(*core[1:]),
            vmem(*core), vmem(*core), vmem(*core[1:]),
            vmem(1, 1, cols), vmem(total, 1, cols),
            pltpu.SemaphoreType.DMA((4,)),
            pltpu.SemaphoreType.DMA((8,)), pltpu.SemaphoreType.DMA((8,)),
            pltpu.SemaphoreType.DMA((3,)), pltpu.SemaphoreType.DMA((3,)),
            pltpu.SemaphoreType.DMA, pltpu.SemaphoreType.DMA,
        ],
        compiler_params=pltpu.CompilerParams(
            collective_id=0, has_side_effects=True, vmem_limit_bytes=40 * 1024 * 1024),
        name="picard",
    )(friction_rows, u_prior, friction_table, bed_fixed, ice_mask)


def solution(mesh):
    sizes = (mesh.shape["plane"], mesh.shape["planey"], mesh.shape["ens"])
    in_specs = (
        P(("group", "ens"), None, None, "plane", "planey"),
        P(("group", "ens")),
        P("group", "plane", "planey"),
        P("plane", "planey"),
        P("plane", "planey"),
    )
    out_specs = P("group", None, "plane", "planey")
    return jax.shard_map(functools.partial(body, sizes), mesh=mesh, in_specs=in_specs,
                         out_specs=out_specs, check_vma=False)
```

```python
import functools
import jax
import jax.numpy as jnp
from jax import lax
from jax.experimental import pallas as pl
from jax.experimental.pallas import tpu as pltpu
from jax.sharding import PartitionSpec as P

bed_unit = 2.0 ** (-29)
HALO = 4
SLOTS = 16
STEP_I = (0.25, 0.125)
STEP_J = (0.125, 0.25)


def iota(shape, dim):
    return lax.broadcasted_iota(jnp.int32, shape, dim)


def shift_i(x, step):
    return pltpu.roll(x, (-step) % x.shape[-2], x.ndim - 2)


def shift_j(x, step):
    rolled = pltpu.roll(x, (-step) % x.shape[-1], x.ndim - 1)
    swapped = jnp.concatenate([rolled[1:2], rolled[0:1]], axis=0)
    lane = iota(x.shape, x.ndim - 1)
    edge = 0 if step < 0 else x.shape[-1] - 1
    return jnp.where(lane == edge, swapped, rolled)


def spread_ij(x, c):
    x = x + STEP_I[c] * (shift_i(x, 1) + shift_i(x, -1))
    return x + STEP_J[c] * (shift_j(x, 1) + shift_j(x, -1))


def spread_z(ref, index, z):
    return ref[index + (z + 1,)] + 0.5 * (ref[index + (z,)] + ref[index + (z + 2,)])


def kernel(sizes, rows_hbm, u_hbm, table_hbm, bed_hbm, mask_hbm, out_ref,
           rows_ref, u_v, table_v, bed_v, mask_v,
           up_s, down_s, side_s, corner_s,
           below_r, above_r, side_r, corner_r, hx,
           ext, roots, tr, pa, pb, r_ext, a_ext, force,
           r_core, a_core, w_core, r_peer, a_peer, w_peer,
           gram_s, gram_r,
           relay, in_sem, halo_send, halo_recv, peer_send, peer_recv, gram_send, gram_recv):
    np_, nq, ne = sizes
    members, _, layers, rows, cols = u_v.shape
    ring = rows + 2 * HALO
    ix, iy, ie = lax.axis_index("plane"), lax.axis_index("planey"), lax.axis_index("ens")

    total = np_ * nq * ne
    mesh_id = pl.DeviceIdType.MESH

    adjacent = []
    for dx in (0, -1, 1):
        for dy in (0, -1, 1):
            for de in range(ne):
                if (dx, dy, de) == (0, 0, 0):
                    continue
                tx, ty = ix + dx, iy + dy
                ok = (tx >= 0) & (tx < np_) & (ty >= 0) & (ty < nq)
                where = {"plane": jnp.clip(tx, 0, np_ - 1), "planey": jnp.clip(ty, 0, nq - 1),
                         "ens": lax.rem(ie + de, ne)}
                adjacent.append((ok, where))
    span_x = 1 + (ix > 0).astype(jnp.int32) + (ix < np_ - 1).astype(jnp.int32)
    span_y = 1 + (iy > 0).astype(jnp.int32) + (iy < nq - 1).astype(jnp.int32)
    adjacent_count = span_x * span_y * ne - 1
    rounds = max(max(np_, nq) - 2, 0)

    def signal_adjacent(sem):
        for ok, where in adjacent:
            @pl.when(ok)
            def _(where=where):
                pl.semaphore_signal(sem, inc=1, device_id=where, device_id_type=mesh_id)

    barrier = pltpu.get_barrier_semaphore()
    signal_adjacent(barrier)

    loads = [
        pltpu.make_async_copy(src, dst, in_sem.at[i])
        for i, (src, dst) in enumerate(
            ((u_hbm, u_v), (table_hbm, table_v), (bed_hbm, bed_v), (mask_hbm, mask_v),
             (rows_hbm, rows_ref))
        )
    ]
    for load in loads:
        load.start()

    def group_target(d):
        de, rest = d // (np_ * nq), d % (np_ * nq)
        return {
            "plane": lax.rem(ix + rest // nq, np_),
            "planey": lax.rem(iy + rest % nq, nq),
            "ens": lax.rem(ie + de, ne),
        }

    def each_peer(fn):
        if total <= 32:
            for d in range(1, total):
                fn(d)
        else:
            def step(d, carry):
                fn(d)
                return carry
            lax.fori_loop(1, total, step, 0)

    flows = []
    for i, (dx, dy, src, dst) in enumerate((
        (-1, 0, up_s, below_r),
        (1, 0, down_s, above_r),
        (0, -1, side_s, side_r.at[1]),
        (0, 1, side_s, side_r.at[0]),
        (-1, -1, corner_s, corner_r.at[0, 1]),
        (-1, 1, corner_s, corner_r.at[0, 0]),
        (1, -1, corner_s, corner_r.at[1, 1]),
        (1, 1, corner_s, corner_r.at[1, 0]),
    )):
        tx, ty = ix + dx, iy + dy
        sx, sy = ix - dx, iy - dy
        to_ok = (tx >= 0) & (tx < np_) & (ty >= 0) & (ty < nq)
        from_ok = (sx >= 0) & (sx < np_) & (sy >= 0) & (sy < nq)
        copy = pltpu.make_async_remote_copy(
            src_ref=src, dst_ref=dst, send_sem=halo_send.at[i], recv_sem=halo_recv.at[i],
            device_id={"plane": jnp.clip(tx, 0, np_ - 1), "planey": jnp.clip(ty, 0, nq - 1)},
            device_id_type=pl.DeviceIdType.MESH)
        flows.append((copy, to_ok, from_ok, dst))

    for load in loads:
        load.wait()

    planes = [(lambda m=m, c=c, z=z: u_v[m, c, z])
              for m in range(members) for z in range(layers) for c in range(2)]
    first_extra = len(planes)
    planes.append(lambda: bed_v[...].astype(jnp.float32) * bed_unit)
    planes.append(lambda: mask_v[...].astype(jnp.float32))
    for m in range(members):
        planes.append(lambda m=m: table_v[rows_ref[m]])
    if len(planes) % 2:
        planes.append(planes[-1])
    groups = side_s.shape[0]

    low8 = iota((8, cols), 0) < 4
    lane_x = iota((rows, cols), 1)
    for g in range(groups):
        packed = jnp.zeros((rows, cols), jnp.float32)
        for k in range(SLOTS):
            p = g * SLOTS + k
            if p >= len(planes):
                continue
            rolled = pltpu.roll(planes[p](), (8 * k + 4) % cols, 1)
            packed = jnp.where((lane_x // 8) == k, rolled, packed)
        side_s[g] = packed
        corner_s[g] = jnp.where(low8, packed[0:8], packed[rows - 8:rows])

    def ends(value):
        return jnp.where(low8, value[0:8], value[rows - 8:rows])

    for i in range(len(planes) // 2):
        first = ends(planes[2 * i]())
        turned = pltpu.roll(ends(planes[2 * i + 1]()), 4, 0)
        up_s[i] = jnp.where(low8, first, turned)
        down_s[i] = jnp.where(low8, turned, first)

    pl.semaphore_wait(barrier, adjacent_count)
    for copy, to_ok, from_ok, dst in flows:
        pl.when(to_ok)(copy.start)
    if rounds > 0:
        signal_adjacent(relay.at[0])

    for copy, to_ok, from_ok, dst in flows:
        @pl.when(jnp.logical_not(from_ok))
        def _(dst=dst):
            dst[...] = jnp.zeros(dst.shape, jnp.float32)
    zero = jnp.zeros((2, ring, cols), jnp.float32)
    for m in range(members):
        for end in (0, layers + 1):
            roots[m, end] = zero
            for c in range(2):
                ext[m, c, end] = zero
                pa[m, c, end] = zero
                pb[m, c, end] = zero
    cover_core = mask_v[...].astype(jnp.float32)
    for c in range(2):
        for z in range(layers):
            summed = u_v[0, c, z]
            for m in range(1, members):
                summed = summed + u_v[m, c, z]
            w_core[c, z] = cover_core * summed

    for copy, to_ok, from_ok, dst in flows:
        pl.when(from_ok)(copy.wait_recv)

    lane_h = iota((rows, cols), 1)
    lane_8 = iota((8, cols), 1)
    for g in range(groups):
        hx[g, 0:rows] = jnp.where(lane_h % 8 < 4, side_r[0, g], side_r[1, g])
        left = jnp.where(low8, corner_r[0, 0, g], corner_r[1, 0, g])
        right = jnp.where(low8, corner_r[0, 1, g], corner_r[1, 1, g])
        hx[g, rows:ring] = jnp.where(lane_8 % 8 < 4, left, right)

    def tail(p):
        i = p // 2
        if p % 2 == 0:
            return jnp.where(low8, below_r[i], above_r[i])
        return pltpu.roll(jnp.where(low8, above_r[i], below_r[i]), 4, 0)

    def extended(p):
        core = jnp.concatenate([planes[p](), tail(p)], axis=0)
        k = p % SLOTS
        halo = pltpu.roll(hx[p // SLOTS], (-(8 * k + 4)) % cols, 1)
        return jnp.stack([core, halo])

    p = 0
    for m in range(members):
        for z in range(layers):
            for c in range(2):
                ext[m, c, z + 1] = extended(p)
                p += 1
    bed = extended(first_extra)
    cover = extended(first_extra + 1)
    row = iota((2, ring, cols), 1)
    position = (ix * rows + jnp.where(row < rows + HALO, row, row - ring)).astype(jnp.float32)
    thickness = 1.0 + 2.0 * position / (np_ * rows - 1)
    slope_x = (shift_i(bed, 1) - shift_i(bed, -1)) * 0.5
    slope_y = (shift_j(bed, 1) - shift_j(bed, -1)) * 0.5
    force[0] = -(cover * thickness * slope_x)
    force[1] = -(cover * thickness * slope_y)
    force[2] = cover
    for m in range(members):
        force[3 + m] = cover * extended(first_extra + 2 + m)

    def roots_step(z, carry):
        cover = force[2]
        for m in range(members):
            u, v = ext[m, 0, z + 1], ext[m, 1, z + 1]
            u_i = (shift_i(u, 1) - shift_i(u, -1)) * 0.5
            v_j = (shift_j(v, 1) - shift_j(v, -1)) * 0.5
            shear = ((shift_j(u, 1) - shift_j(u, -1)) + (shift_i(v, 1) - shift_i(v, -1))) * 0.5
            u_z = (ext[m, 0, z + 2] - ext[m, 0, z]) * 0.5
            v_z = (ext[m, 1, z + 2] - ext[m, 1, z]) * 0.5
            strain = (u_i * u_i + v_j * v_j + u_i * v_j + 0.25 * shear * shear
                      + 0.25 * (u_z * u_z + v_z * v_z))
            root = cover * jnp.exp(jnp.log(strain + 0.1) * (-1.0 / 6.0))
            roots[m, z + 1] = root
            pa[m, 0, z + 1] = root * u
            pa[m, 1, z + 1] = root * v
        return carry

    lax.fori_loop(0, layers, roots_step, 0, unroll=2)
    for k in range(1, rounds):
        pl.semaphore_wait(relay.at[k - 1], adjacent_count)
        signal_adjacent(relay.at[k])

    def image(m, c, z, field, p_ref):
        across = tr[m, c, z]
        bottom = jnp.where(z == 0, 1.0, 0.0).astype(jnp.float32)
        diag = force[3 + m] * bottom + (1.0 - force[2])
        spread = spread_ij(spread_z(p_ref, (m, c), z), c)
        return 4.0 * roots[m, z + 1] * (across * field - spread) + diag * field

    zero_core = jnp.zeros((rows, cols), jnp.float32)

    def residual_step(z, carry):
        carry = list(carry)
        for m in range(members):
            near = spread_z(roots, (m,), z)
            for c in range(2):
                tr[m, c, z] = spread_ij(near, c)
                start = force[2] * ext[m, c, z + 1]
                r = force[c] - image(m, c, z, start, pa)
                r_ext[m, c, z] = r
                pb[m, c, z + 1] = roots[m, z + 1] * r
                core = r[0, 0:rows]
                r_core[m, c, z] = core
                carry[m] = carry[m] + core * core
        return tuple(carry)

    rr = lax.fori_loop(0, layers, residual_step, (zero_core,) * members, unroll=2)

    peer = {"ens": lax.rem(ie + 1, ne)}

    def to_peer(i, src, dst):
        return pltpu.make_async_remote_copy(
            src_ref=src, dst_ref=dst, send_sem=peer_send.at[i], recv_sem=peer_recv.at[i],
            device_id=peer, device_id_type=pl.DeviceIdType.MESH)

    peer_flows = [to_peer(0, w_core, w_peer), to_peer(1, r_core, r_peer), to_peer(2, a_core, a_peer)]
    peer_flows[0].start()

    def image_step(z, carry):
        carry = list(carry)
        for m in range(members):
            for c in range(2):
                r = r_ext[m, c, z]
                a = image(m, c, z, r, pb)
                a_ext[m, c, z] = a
                pa[m, c, z + 1] = roots[m, z + 1] * a
                core = a[0, 0:rows]
                a_core[m, c, z] = core
                carry[2 * m] = carry[2 * m] + r[0, 0:rows] * core
                carry[2 * m + 1] = carry[2 * m + 1] + core * core
        return tuple(carry)

    ra_aa = lax.fori_loop(0, layers, image_step, (zero_core,) * (2 * members), unroll=2)
    peer_flows[1].start()

    def second_step(z, carry):
        carry = list(carry)
        for m in range(members):
            for c in range(2):
                a = a_ext[m, c, z]
                b = image(m, c, z, a, pa)
                carry[m] = carry[m] + a[0, 0:rows] * b[0, 0:rows]
        return tuple(carry)

    ab = lax.fori_loop(0, layers, second_step, (zero_core,) * members, unroll=2)
    peer_flows[2].start()

    lane_1 = iota((1, cols), 1)
    mine = jnp.zeros((1, cols), jnp.float32)
    for m in range(members):
        for q, acc in enumerate((rr[m], ra_aa[2 * m], ra_aa[2 * m + 1], ab[m])):
            value = jnp.sum(jnp.sum(acc, axis=0, keepdims=True), axis=1, keepdims=True)
            mine = jnp.where(lane_1 == 4 * m + q, value, mine)
    gram_s[0] = mine

    if rounds > 0:
        pl.semaphore_wait(relay.at[rounds - 1], adjacent_count)

    def gram_copy(d):
        return pltpu.make_async_remote_copy(
            src_ref=gram_s, dst_ref=gram_r.at[pl.ds(d, 1)],
            send_sem=gram_send, recv_sem=gram_recv,
            device_id=group_target(d), device_id_type=pl.DeviceIdType.MESH)

    each_peer(lambda d: gram_copy(d).start())
    everything = pltpu.make_async_remote_copy(
        src_ref=gram_r.at[pl.ds(1, total - 1)], dst_ref=gram_r.at[pl.ds(1, total - 1)],
        send_sem=gram_send, recv_sem=gram_recv,
        device_id=group_target(1), device_id_type=pl.DeviceIdType.MESH)
    everything.wait_recv()

    half = np_ * nq
    own = mine
    if half > 1:
        own = own + jnp.sum(gram_r[1:half], axis=0)
    sums = [own] + [jnp.sum(gram_r[half * e:half * (e + 1)], axis=0) for e in range(1, ne)]
    steps = []
    for e in range(ne):
        for m in range(members):
            g_rr, g_ra, g_aa, g_ab = [
                jnp.sum(jnp.where(lane_1 == 4 * m + q, sums[e], 0.0), axis=1, keepdims=True)
                for q in range(4)
            ]
            first = g_rr / g_ra
            following = g_rr - 2.0 * first * g_ra + first * first * g_aa
            growth = 1.0 + following / g_rr
            curve = (growth * growth * g_ra - 2.0 * growth * first * g_aa
                     + first * first * g_ab)
            second = following / curve
            share = 1.0 / (members * ne)
            steps.append(((first + second * growth) * share, second * first * share))

    for flow in peer_flows:
        flow.wait_recv()
    share = 1.0 / (members * ne)

    def final_step(z, carry):
        for c in range(2):
            value = share * (w_core[c, z] + w_peer[c, z])
            for m in range(members):
                value = value + steps[m][0] * r_core[m, c, z] - steps[m][1] * a_core[m, c, z]
                one, two = steps[members + m]
                value = value + one * r_peer[m, c, z] - two * a_peer[m, c, z]
            out_ref[c, z] = value
        return carry

    lax.fori_loop(0, layers, final_step, 0)

    for copy, to_ok, from_ok, dst in flows:
        pl.when(to_ok)(copy.wait_send)
    for flow in peer_flows:
        flow.wait_send()
    everything.wait_send()


def body(sizes, u_prior, friction_rows, friction_table, bed_fixed, ice_mask):
    members, _, layers, rows, cols = u_prior.shape
    levels = friction_table.shape[0]
    total = sizes[0] * sizes[1] * sizes[2]
    ring = rows + 2 * HALO
    planes = members * layers * 2 + 2 + members
    pairs = (planes + 1) // 2
    groups = (2 * pairs + SLOTS - 1) // SLOTS
    f32 = jnp.float32
    any_space = pl.BlockSpec(memory_space=pl.ANY)
    vmem = lambda *shape: pltpu.VMEM(shape, f32)
    core = (members, 2, layers, rows, cols)
    wide = (2, ring, cols)
    return pl.pallas_call(
        functools.partial(kernel, sizes),
        out_shape=jax.ShapeDtypeStruct((2, layers, rows, cols), f32),
        in_specs=[any_space] * 5,
        out_specs=pl.BlockSpec(memory_space=pltpu.VMEM),
        scratch_shapes=[
            pltpu.SMEM((members,), jnp.int32), vmem(*core), vmem(levels, rows, cols),
            pltpu.VMEM((rows, cols), jnp.int32), pltpu.VMEM((rows, cols), jnp.int32),
            vmem(pairs, 8, cols), vmem(pairs, 8, cols), vmem(groups, rows, cols), vmem(groups, 8, cols),
            vmem(pairs, 8, cols), vmem(pairs, 8, cols), vmem(2, groups, rows, cols),
            vmem(2, 2, groups, 8, cols), vmem(groups, ring, cols),
            vmem(members, 2, layers + 2, *wide), vmem(members, layers + 2, *wide),
            vmem(members, 2, layers, *wide),
            vmem(members, 2, layers + 2, *wide), vmem(members, 2, layers + 2, *wide),
            vmem(members, 2, layers, *wide), vmem(members, 2, layers, *wide),
            vmem(3 + members, *wide),
            vmem(*core), vmem(*core), vmem(*core[1:]),
            vmem(*core), vmem(*core), vmem(*core[1:]),
            vmem(1, 1, cols), vmem(total, 1, cols),
            pltpu.SemaphoreType.REGULAR((max(sizes[0], sizes[1]),)),
            pltpu.SemaphoreType.DMA((5,)),
            pltpu.SemaphoreType.DMA((8,)), pltpu.SemaphoreType.DMA((8,)),
            pltpu.SemaphoreType.DMA((3,)), pltpu.SemaphoreType.DMA((3,)),
            pltpu.SemaphoreType.DMA, pltpu.SemaphoreType.DMA,
        ],
        compiler_params=pltpu.CompilerParams(
            collective_id=0, has_side_effects=True),
        name="picard",
    )(friction_rows, u_prior, friction_table, bed_fixed, ice_mask)


def solution(mesh):
    sizes = (mesh.shape["plane"], mesh.shape["planey"], mesh.shape["ens"])
    in_specs = (
        P(("group", "ens"), None, None, "plane", "planey"),
        P(("group", "ens")),
        P("group", "plane", "planey"),
        P("plane", "planey"),
        P("plane", "planey"),
    )
    out_specs = P("group", None, "plane", "planey")
    return jax.shard_map(functools.partial(body, sizes), mesh=mesh, in_specs=in_specs,
                         out_specs=out_specs, check_vma=False)
```

```python
import functools
import jax
import jax.numpy as jnp
from jax import lax
from jax.experimental import pallas as pl
from jax.experimental.pallas import tpu as pltpu
from jax.sharding import PartitionSpec as P

bed_unit = 2.0 ** (-29)
HALO = 4
SLOTS = 16
STEP_I = (0.25, 0.125)
STEP_J = (0.125, 0.25)


def iota(shape, dim):
    return lax.broadcasted_iota(jnp.int32, shape, dim)


def shift_i(x, step):
    return pltpu.roll(x, (-step) % x.shape[-2], x.ndim - 2)


def shift_j(x, step):
    rolled = pltpu.roll(x, (-step) % x.shape[-1], x.ndim - 1)
    swapped = jnp.concatenate([rolled[1:2], rolled[0:1]], axis=0)
    lane = iota(x.shape, x.ndim - 1)
    edge = 0 if step < 0 else x.shape[-1] - 1
    return jnp.where(lane == edge, swapped, rolled)


def spread_ij(x, c):
    x = x + STEP_I[c] * (shift_i(x, 1) + shift_i(x, -1))
    return x + STEP_J[c] * (shift_j(x, 1) + shift_j(x, -1))


def spread_z(ref, index, z):
    return ref[index + (z + 1,)] + 0.5 * (ref[index + (z,)] + ref[index + (z + 2,)])


def chunk_places(members, layers):
    chunks, places, pair, group = [], [], 0, 0
    for m in range(members):
        base = 2 + members if m == 0 else 0
        base_even = base + base % 2
        count = base_even + 2 * layers
        pairs, groups = count // 2, (count + SLOTS - 1) // SLOTS
        chunks.append((pair, pairs, group, groups))
        places.append(base_even)
        pair, group = pair + pairs, group + groups
    return chunks, places


def kernel(sizes, rows_hbm, u_hbm, table_hbm, bed_hbm, mask_hbm, out_ref,
           rows_ref, u_v, table_v, bed_v, mask_v,
           up_s, down_s, side_s, corner_s,
           below_r, above_r, side_r, corner_r, hx,
           ext, roots, tr, pa, pb, r_ext, a_ext, force,
           r_core, a_core, w_core, r_peer, a_peer, w_peer,
           gram_s, gram_r,
           relay, in_sem, halo_send, halo_recv, peer_send, peer_recv, gram_send, gram_recv):
    np_, nq, ne = sizes
    members, _, layers, rows, cols = u_v.shape
    ring = rows + 2 * HALO
    ix, iy, ie = lax.axis_index("plane"), lax.axis_index("planey"), lax.axis_index("ens")

    total = np_ * nq * ne
    mesh_id = pl.DeviceIdType.MESH

    adjacent = []
    for dx in (0, -1, 1):
        for dy in (0, -1, 1):
            for de in range(ne):
                if (dx, dy, de) == (0, 0, 0):
                    continue
                tx, ty = ix + dx, iy + dy
                ok = (tx >= 0) & (tx < np_) & (ty >= 0) & (ty < nq)
                where = {"plane": jnp.clip(tx, 0, np_ - 1), "planey": jnp.clip(ty, 0, nq - 1),
                         "ens": lax.rem(ie + de, ne)}
                adjacent.append((ok, where))
    span_x = 1 + (ix > 0).astype(jnp.int32) + (ix < np_ - 1).astype(jnp.int32)
    span_y = 1 + (iy > 0).astype(jnp.int32) + (iy < nq - 1).astype(jnp.int32)
    adjacent_count = span_x * span_y * ne - 1
    rounds = max(max(np_, nq) - 2, 0)

    def signal_adjacent(sem):
        for ok, where in adjacent:
            @pl.when(ok)
            def _(where=where):
                pl.semaphore_signal(sem, inc=1, device_id=where, device_id_type=mesh_id)

    barrier = pltpu.get_barrier_semaphore()
    signal_adjacent(barrier)

    loads = [
        pltpu.make_async_copy(src, dst, in_sem.at[i])
        for i, (src, dst) in enumerate(
            ((u_hbm, u_v), (table_hbm, table_v), (bed_hbm, bed_v), (mask_hbm, mask_v),
             (rows_hbm, rows_ref))
        )
    ]
    for load in loads:
        load.start()

    def group_target(d):
        de, rest = d // (np_ * nq), d % (np_ * nq)
        return {
            "plane": lax.rem(ix + rest // nq, np_),
            "planey": lax.rem(iy + rest % nq, nq),
            "ens": lax.rem(ie + de, ne),
        }

    def each_peer(fn):
        if total <= 32:
            for d in range(1, total):
                fn(d)
        else:
            def step(d, carry):
                fn(d)
                return carry
            lax.fori_loop(1, total, step, 0)

    shared = [
        lambda: bed_v[...].astype(jnp.float32) * bed_unit,
        lambda: mask_v[...].astype(jnp.float32),
    ] + [(lambda m=m: table_v[rows_ref[m]]) for m in range(members)]
    if len(shared) % 2:
        shared.append(shared[-1])
    chunks, places = chunk_places(members, layers)
    readers = [
        (shared if m == 0 else [])
        + [(lambda m=m, c=c, z=z: u_v[m, c, z]) for z in range(layers) for c in range(2)]
        for m in range(members)
    ]

    flows = [[] for _ in chunks]
    absent = []
    for i, (dx, dy, src, dst) in enumerate((
        (-1, 0, up_s, below_r),
        (1, 0, down_s, above_r),
        (0, -1, side_s, side_r.at[1]),
        (0, 1, side_s, side_r.at[0]),
        (-1, -1, corner_s, corner_r.at[0, 1]),
        (-1, 1, corner_s, corner_r.at[0, 0]),
        (1, -1, corner_s, corner_r.at[1, 1]),
        (1, 1, corner_s, corner_r.at[1, 0]),
    )):
        tx, ty = ix + dx, iy + dy
        sx, sy = ix - dx, iy - dy
        to_ok = (tx >= 0) & (tx < np_) & (ty >= 0) & (ty < nq)
        from_ok = (sx >= 0) & (sx < np_) & (sy >= 0) & (sy < nq)
        absent.append((jnp.logical_not(from_ok), dst))
        for k, (pair, pairs, group, groups) in enumerate(chunks):
            part = pl.ds(pair, pairs) if i < 2 else pl.ds(group, groups)
            copy = pltpu.make_async_remote_copy(
                src_ref=src.at[part], dst_ref=dst.at[part],
                send_sem=halo_send.at[8 * k + i], recv_sem=halo_recv.at[8 * k + i],
                device_id={"plane": jnp.clip(tx, 0, np_ - 1), "planey": jnp.clip(ty, 0, nq - 1)},
                device_id_type=mesh_id)
            flows[k].append((copy, to_ok, from_ok))

    for load in loads:
        load.wait()

    low8 = iota((8, cols), 0) < 4
    lane_x = iota((rows, cols), 1)

    def ends(value):
        return jnp.where(low8, value[0:8], value[rows - 8:rows])

    for (pair, pairs, group, groups), read in zip(chunks, readers):
        for g in range(groups):
            packed = jnp.zeros((rows, cols), jnp.float32)
            for k in range(min(SLOTS, len(read) - g * SLOTS)):
                rolled = pltpu.roll(read[g * SLOTS + k](), (8 * k + 4) % cols, 1)
                packed = jnp.where((lane_x // 8) == k, rolled, packed)
            side_s[group + g] = packed
            corner_s[group + g] = ends(packed)
        for i in range(pairs):
            first = ends(read[2 * i]())
            turned = pltpu.roll(ends(read[min(2 * i + 1, len(read) - 1)]()), 4, 0)
            up_s[pair + i] = jnp.where(low8, first, turned)
            down_s[pair + i] = jnp.where(low8, turned, first)

    pl.semaphore_wait(barrier, adjacent_count)
    for chunk in flows:
        for copy, to_ok, from_ok in chunk:
            pl.when(to_ok)(copy.start)
    if rounds > 0:
        signal_adjacent(relay.at[0])

    for gone, dst in absent:
        @pl.when(gone)
        def _(dst=dst):
            dst[...] = jnp.zeros(dst.shape, jnp.float32)
    zero = jnp.zeros((2, ring, cols), jnp.float32)
    for m in range(members):
        for end in (0, layers + 1):
            roots[m, end] = zero
            for c in range(2):
                ext[m, c, end] = zero
                pa[m, c, end] = zero
                pb[m, c, end] = zero
    cover_core = mask_v[...].astype(jnp.float32)
    for c in range(2):
        for z in range(layers):
            summed = u_v[0, c, z]
            for m in range(1, members):
                summed = summed + u_v[m, c, z]
            w_core[c, z] = cover_core * summed

    def arrive(k):
        for copy, to_ok, from_ok in flows[k]:
            pl.when(from_ok)(copy.wait_recv)
        _, _, group, groups = chunks[k]
        for g in range(group, group + groups):
            hx[g, 0:rows] = jnp.where(lane_x % 8 < 4, side_r[0, g], side_r[1, g])
            left = jnp.where(low8, corner_r[0, 0, g], corner_r[1, 0, g])
            right = jnp.where(low8, corner_r[0, 1, g], corner_r[1, 1, g])
            hx[g, rows:ring] = jnp.where(lane_x[0:8] % 8 < 4, left, right)

    def extended(k, p):
        pair, _, group, _ = chunks[k]
        i = pair + p // 2
        if p % 2 == 0:
            tail = jnp.where(low8, below_r[i], above_r[i])
        else:
            tail = pltpu.roll(jnp.where(low8, above_r[i], below_r[i]), 4, 0)
        core = jnp.concatenate([readers[k][p](), tail], axis=0)
        halo = pltpu.roll(hx[group + p // SLOTS], (-(8 * (p % SLOTS) + 4)) % cols, 1)
        return jnp.stack([core, halo])

    def assemble(m):
        arrive(m)
        base = places[m]
        for z in range(layers):
            for c in range(2):
                ext[m, c, z + 1] = extended(m, base + 2 * z + c)
        if m > 0:
            return
        bed = extended(0, 0)
        cover = extended(0, 1)
        row = iota((2, ring, cols), 1)
        position = (ix * rows + jnp.where(row < rows + HALO, row, row - ring)).astype(jnp.float32)
        thickness = 1.0 + 2.0 * position / (np_ * rows - 1)
        slope_x = (shift_i(bed, 1) - shift_i(bed, -1)) * 0.5
        slope_y = (shift_j(bed, 1) - shift_j(bed, -1)) * 0.5
        force[0] = -(cover * thickness * slope_x)
        force[1] = -(cover * thickness * slope_y)
        force[2] = cover
        for k in range(members):
            force[3 + k] = cover * extended(0, 2 + k)

    def roots_step(m, z):
        u, v = ext[m, 0, z + 1], ext[m, 1, z + 1]
        u_i = (shift_i(u, 1) - shift_i(u, -1)) * 0.5
        v_j = (shift_j(v, 1) - shift_j(v, -1)) * 0.5
        shear = ((shift_j(u, 1) - shift_j(u, -1)) + (shift_i(v, 1) - shift_i(v, -1))) * 0.5
        u_z = (ext[m, 0, z + 2] - ext[m, 0, z]) * 0.5
        v_z = (ext[m, 1, z + 2] - ext[m, 1, z]) * 0.5
        strain = (u_i * u_i + v_j * v_j + u_i * v_j + 0.25 * shear * shear
                  + 0.25 * (u_z * u_z + v_z * v_z))
        root = force[2] * jnp.exp(jnp.log(strain + 0.1) * (-1.0 / 6.0))
        roots[m, z + 1] = root
        pa[m, 0, z + 1] = root * u
        pa[m, 1, z + 1] = root * v

    def image(m, c, z, field, p_ref):
        diag = 1.0 - force[2]
        if z == 0:
            diag = diag + force[3 + m]
        spread = spread_ij(spread_z(p_ref, (m, c), z), c)
        return 4.0 * roots[m, z + 1] * (tr[m, c, z] * field - spread) + diag * field

    def residual_step(m, z, acc):
        near = spread_z(roots, (m,), z)
        for c in range(2):
            tr[m, c, z] = spread_ij(near, c)
            r = force[c] - image(m, c, z, force[2] * ext[m, c, z + 1], pa)
            r_ext[m, c, z] = r
            pb[m, c, z + 1] = roots[m, z + 1] * r
            core = r[0, 0:rows]
            r_core[m, c, z] = core
            acc = acc + core * core
        return acc

    def image_step(m, z, ra, aa):
        for c in range(2):
            r = r_ext[m, c, z]
            a = image(m, c, z, r, pb)
            a_ext[m, c, z] = a
            pa[m, c, z + 1] = roots[m, z + 1] * a
            core = a[0, 0:rows]
            a_core[m, c, z] = core
            ra = ra + r[0, 0:rows] * core
            aa = aa + core * core
        return ra, aa

    def second_step(m, z, ab):
        for c in range(2):
            a = a_ext[m, c, z]
            b = image(m, c, z, a, pa)
            ab = ab + a[0, 0:rows] * b[0, 0:rows]
        return ab

    peer = {"ens": lax.rem(ie + 1, ne)}

    def to_peer(i, src, dst):
        return pltpu.make_async_remote_copy(
            src_ref=src, dst_ref=dst, send_sem=peer_send.at[i], recv_sem=peer_recv.at[i],
            device_id=peer, device_id_type=mesh_id)

    peer_flows = [to_peer(0, w_core, w_peer)]
    for m in range(members):
        peer_flows.append(to_peer(2 * m + 1, r_core.at[m], r_peer.at[m]))
        peer_flows.append(to_peer(2 * m + 2, a_core.at[m], a_peer.at[m]))

    zero_core = jnp.zeros((rows, cols), jnp.float32)
    grams = []
    for m in range(members):
        assemble(m)
        for z in range(layers):
            roots_step(m, z)
        if m == 0:
            peer_flows[0].start()
            for k in range(1, rounds):
                pl.semaphore_wait(relay.at[k - 1], adjacent_count)
                signal_adjacent(relay.at[k])
        rr = ra = aa = ab = zero_core
        for z in range(layers):
            rr = residual_step(m, z, rr)
        for z in range(layers):
            ra, aa = image_step(m, z, ra, aa)
        peer_flows[2 * m + 1].start()
        for z in range(layers):
            ab = second_step(m, z, ab)
        peer_flows[2 * m + 2].start()
        grams.append((rr, ra, aa, ab))

    lane_1 = iota((1, cols), 1)
    mine = jnp.zeros((1, cols), jnp.float32)
    for m in range(members):
        for q, acc in enumerate(grams[m]):
            value = jnp.sum(jnp.sum(acc, axis=0, keepdims=True), axis=1, keepdims=True)
            mine = jnp.where(lane_1 == 4 * m + q, value, mine)
    gram_s[0] = mine

    if rounds > 0:
        pl.semaphore_wait(relay.at[rounds - 1], adjacent_count)

    def gram_copy(d):
        return pltpu.make_async_remote_copy(
            src_ref=gram_s, dst_ref=gram_r.at[pl.ds(d, 1)],
            send_sem=gram_send, recv_sem=gram_recv,
            device_id=group_target(d), device_id_type=pl.DeviceIdType.MESH)

    each_peer(lambda d: gram_copy(d).start())
    everything = pltpu.make_async_remote_copy(
        src_ref=gram_r.at[pl.ds(1, total - 1)], dst_ref=gram_r.at[pl.ds(1, total - 1)],
        send_sem=gram_send, recv_sem=gram_recv,
        device_id=group_target(1), device_id_type=pl.DeviceIdType.MESH)
    everything.wait_recv()

    half = np_ * nq
    own = mine
    if half > 1:
        own = own + jnp.sum(gram_r[1:half], axis=0)
    sums = [own] + [jnp.sum(gram_r[half * e:half * (e + 1)], axis=0) for e in range(1, ne)]
    steps = []
    for e in range(ne):
        for m in range(members):
            g_rr, g_ra, g_aa, g_ab = [
                jnp.sum(jnp.where(lane_1 == 4 * m + q, sums[e], 0.0), axis=1, keepdims=True)
                for q in range(4)
            ]
            first = g_rr / g_ra
            following = g_rr - 2.0 * first * g_ra + first * first * g_aa
            growth = 1.0 + following / g_rr
            curve = (growth * growth * g_ra - 2.0 * growth * first * g_aa
                     + first * first * g_ab)
            second = following / curve
            share = 1.0 / (members * ne)
            steps.append(((first + second * growth) * share, second * first * share))

    for flow in peer_flows:
        flow.wait_recv()
    share = 1.0 / (members * ne)

    def final_step(z, carry):
        for c in range(2):
            value = share * (w_core[c, z] + w_peer[c, z])
            for m in range(members):
                value = value + steps[m][0] * r_core[m, c, z] - steps[m][1] * a_core[m, c, z]
                one, two = steps[members + m]
                value = value + one * r_peer[m, c, z] - two * a_peer[m, c, z]
            out_ref[c, z] = value
        return carry

    lax.fori_loop(0, layers, final_step, 0)

    for chunk in flows:
        for copy, to_ok, from_ok in chunk:
            pl.when(to_ok)(copy.wait_send)
    for flow in peer_flows:
        flow.wait_send()
    everything.wait_send()


def body(sizes, u_prior, friction_rows, friction_table, bed_fixed, ice_mask):
    members, _, layers, rows, cols = u_prior.shape
    levels = friction_table.shape[0]
    total = sizes[0] * sizes[1] * sizes[2]
    ring = rows + 2 * HALO
    chunks, _ = chunk_places(members, layers)
    pairs = sum(chunk[1] for chunk in chunks)
    groups = sum(chunk[3] for chunk in chunks)
    f32 = jnp.float32
    any_space = pl.BlockSpec(memory_space=pl.ANY)
    vmem = lambda *shape: pltpu.VMEM(shape, f32)
    core = (members, 2, layers, rows, cols)
    wide = (2, ring, cols)
    return pl.pallas_call(
        functools.partial(kernel, sizes),
        out_shape=jax.ShapeDtypeStruct((2, layers, rows, cols), f32),
        in_specs=[any_space] * 5,
        out_specs=pl.BlockSpec(memory_space=pltpu.VMEM),
        scratch_shapes=[
            pltpu.SMEM((members,), jnp.int32), vmem(*core), vmem(levels, rows, cols),
            pltpu.VMEM((rows, cols), jnp.int32), pltpu.VMEM((rows, cols), jnp.int32),
            vmem(pairs, 8, cols), vmem(pairs, 8, cols), vmem(groups, rows, cols), vmem(groups, 8, cols),
            vmem(pairs, 8, cols), vmem(pairs, 8, cols), vmem(2, groups, rows, cols),
            vmem(2, 2, groups, 8, cols), vmem(groups, ring, cols),
            vmem(members, 2, layers + 2, *wide), vmem(members, layers + 2, *wide),
            vmem(members, 2, layers, *wide),
            vmem(members, 2, layers + 2, *wide), vmem(members, 2, layers + 2, *wide),
            vmem(members, 2, layers, *wide), vmem(members, 2, layers, *wide),
            vmem(3 + members, *wide),
            vmem(*core), vmem(*core), vmem(*core[1:]),
            vmem(*core), vmem(*core), vmem(*core[1:]),
            vmem(1, 1, cols), vmem(total, 1, cols),
            pltpu.SemaphoreType.REGULAR((max(sizes[0], sizes[1]),)),
            pltpu.SemaphoreType.DMA((5,)),
            pltpu.SemaphoreType.DMA((8 * members,)), pltpu.SemaphoreType.DMA((8 * members,)),
            pltpu.SemaphoreType.DMA((2 * members + 1,)), pltpu.SemaphoreType.DMA((2 * members + 1,)),
            pltpu.SemaphoreType.DMA, pltpu.SemaphoreType.DMA,
        ],
        compiler_params=pltpu.CompilerParams(
            collective_id=0, has_side_effects=True),
        name="picard",
    )(friction_rows, u_prior, friction_table, bed_fixed, ice_mask)


def solution(mesh):
    sizes = (mesh.shape["plane"], mesh.shape["planey"], mesh.shape["ens"])
    in_specs = (
        P(("group", "ens"), None, None, "plane", "planey"),
        P(("group", "ens")),
        P("group", "plane", "planey"),
        P("plane", "planey"),
        P("plane", "planey"),
    )
    out_specs = P("group", None, "plane", "planey")
    return jax.shard_map(functools.partial(body, sizes), mesh=mesh, in_specs=in_specs,
                         out_specs=out_specs, check_vma=False)
```

```python
import functools
import jax
import jax.numpy as jnp
from jax import lax
from jax.experimental import pallas as pl
from jax.experimental.pallas import tpu as pltpu
from jax.sharding import PartitionSpec as P

bed_unit = 2.0 ** (-29)
HALO = 4
SLOTS = 16
STEP_I = (0.25, 0.125)
STEP_J = (0.125, 0.25)


def iota(shape, dim):
    return lax.broadcasted_iota(jnp.int32, shape, dim)


def shift_i(x, step):
    return pltpu.roll(x, (-step) % x.shape[-2], x.ndim - 2)


def shift_j(x, step):
    rolled = pltpu.roll(x, (-step) % x.shape[-1], x.ndim - 1)
    swapped = jnp.concatenate([rolled[1:2], rolled[0:1]], axis=0)
    lane = iota(x.shape, x.ndim - 1)
    edge = 0 if step < 0 else x.shape[-1] - 1
    return jnp.where(lane == edge, swapped, rolled)


def spread_ij(x, c):
    x = x + STEP_I[c] * (shift_i(x, 1) + shift_i(x, -1))
    return x + STEP_J[c] * (shift_j(x, 1) + shift_j(x, -1))


def spread_z(ref, index, z):
    return ref[index + (z + 1,)] + 0.5 * (ref[index + (z,)] + ref[index + (z + 2,)])


def chunk_places(members, layers):
    chunks, places, pair, group = [], [], 0, 0
    for m in range(members):
        base = 2 + members if m == 0 else 0
        base_even = base + base % 2
        count = base_even + 2 * layers
        pairs, groups = count // 2, (count + SLOTS - 1) // SLOTS
        chunks.append((pair, pairs, group, groups))
        places.append(base_even)
        pair, group = pair + pairs, group + groups
    return chunks, places


def kernel(sizes, rows_hbm, u_hbm, table_hbm, bed_hbm, mask_hbm, out_ref,
           rows_ref, u_v, table_v, bed_v, mask_v,
           up_s, down_s, side_s, corner_s,
           below_r, above_r, side_r, corner_r, hx,
           ext, roots, tr, pa, pb, r_ext, a_ext, force,
           r_core, a_core, w_core, r_peer, a_peer, w_peer,
           gram_s, gram_r,
           relay, in_sem, halo_send, halo_recv, peer_send, peer_recv, gram_send, gram_recv):
    np_, nq, ne = sizes
    members, _, layers, rows, cols = u_v.shape
    ring = rows + 2 * HALO
    ix, iy, ie = lax.axis_index("plane"), lax.axis_index("planey"), lax.axis_index("ens")

    total = np_ * nq * ne
    mesh_id = pl.DeviceIdType.MESH

    adjacent = []
    for dx in (0, -1, 1):
        for dy in (0, -1, 1):
            for de in range(ne):
                if (dx, dy, de) == (0, 0, 0):
                    continue
                tx, ty = ix + dx, iy + dy
                ok = (tx >= 0) & (tx < np_) & (ty >= 0) & (ty < nq)
                where = {"plane": jnp.clip(tx, 0, np_ - 1), "planey": jnp.clip(ty, 0, nq - 1),
                         "ens": lax.rem(ie + de, ne)}
                adjacent.append((ok, where))
    span_x = 1 + (ix > 0).astype(jnp.int32) + (ix < np_ - 1).astype(jnp.int32)
    span_y = 1 + (iy > 0).astype(jnp.int32) + (iy < nq - 1).astype(jnp.int32)
    adjacent_count = span_x * span_y * ne - 1
    rounds = max(max(np_, nq) - 2, 0)

    def signal_adjacent(sem):
        for ok, where in adjacent:
            @pl.when(ok)
            def _(where=where):
                pl.semaphore_signal(sem, inc=1, device_id=where, device_id_type=mesh_id)

    barrier = pltpu.get_barrier_semaphore()
    signal_adjacent(barrier)

    loads = [
        pltpu.make_async_copy(src, dst, in_sem.at[i])
        for i, (src, dst) in enumerate(
            ((u_hbm, u_v), (table_hbm, table_v), (bed_hbm, bed_v), (mask_hbm, mask_v),
             (rows_hbm, rows_ref))
        )
    ]
    for load in loads:
        load.start()

    def group_target(d):
        de, rest = d // (np_ * nq), d % (np_ * nq)
        return {
            "plane": lax.rem(ix + rest // nq, np_),
            "planey": lax.rem(iy + rest % nq, nq),
            "ens": lax.rem(ie + de, ne),
        }

    def each_peer(fn):
        if total <= 32:
            for d in range(1, total):
                fn(d)
        else:
            def step(d, carry):
                fn(d)
                return carry
            lax.fori_loop(1, total, step, 0)

    shared = [
        lambda: bed_v[...].astype(jnp.float32) * bed_unit,
        lambda: mask_v[...].astype(jnp.float32),
    ] + [(lambda m=m: table_v[rows_ref[m]]) for m in range(members)]
    if len(shared) % 2:
        shared.append(shared[-1])
    chunks, places = chunk_places(members, layers)
    readers = [
        (shared if m == 0 else [])
        + [(lambda m=m, c=c, z=z: u_v[m, c, z]) for z in range(layers) for c in range(2)]
        for m in range(members)
    ]

    flows = [[] for _ in chunks]
    absent = []
    for i, (dx, dy, src, dst) in enumerate((
        (-1, 0, up_s, below_r),
        (1, 0, down_s, above_r),
        (0, -1, side_s, side_r.at[1]),
        (0, 1, side_s, side_r.at[0]),
        (-1, -1, corner_s, corner_r.at[0, 1]),
        (-1, 1, corner_s, corner_r.at[0, 0]),
        (1, -1, corner_s, corner_r.at[1, 1]),
        (1, 1, corner_s, corner_r.at[1, 0]),
    )):
        tx, ty = ix + dx, iy + dy
        sx, sy = ix - dx, iy - dy
        to_ok = (tx >= 0) & (tx < np_) & (ty >= 0) & (ty < nq)
        from_ok = (sx >= 0) & (sx < np_) & (sy >= 0) & (sy < nq)
        absent.append((jnp.logical_not(from_ok), dst))
        for k, (pair, pairs, group, groups) in enumerate(chunks):
            part = pl.ds(pair, pairs) if i < 2 else pl.ds(group, groups)
            copy = pltpu.make_async_remote_copy(
                src_ref=src.at[part], dst_ref=dst.at[part],
                send_sem=halo_send.at[8 * k + i], recv_sem=halo_recv.at[8 * k + i],
                device_id={"plane": jnp.clip(tx, 0, np_ - 1), "planey": jnp.clip(ty, 0, nq - 1)},
                device_id_type=mesh_id)
            flows[k].append((copy, to_ok, from_ok))

    for load in loads:
        load.wait()

    low8 = iota((8, cols), 0) < 4
    lane_x = iota((rows, cols), 1)

    def ends(value):
        return jnp.where(low8, value[0:8], value[rows - 8:rows])

    for (pair, pairs, group, groups), read in zip(chunks, readers):
        for g in range(groups):
            packed = jnp.zeros((rows, cols), jnp.float32)
            for k in range(min(SLOTS, len(read) - g * SLOTS)):
                rolled = pltpu.roll(read[g * SLOTS + k](), (8 * k + 4) % cols, 1)
                packed = jnp.where((lane_x // 8) == k, rolled, packed)
            side_s[group + g] = packed
            corner_s[group + g] = ends(packed)
        for i in range(pairs):
            first = ends(read[2 * i]())
            turned = pltpu.roll(ends(read[min(2 * i + 1, len(read) - 1)]()), 4, 0)
            up_s[pair + i] = jnp.where(low8, first, turned)
            down_s[pair + i] = jnp.where(low8, turned, first)

    pl.semaphore_wait(barrier, adjacent_count)
    for chunk in flows:
        for copy, to_ok, from_ok in chunk:
            pl.when(to_ok)(copy.start)
    if rounds > 0:
        signal_adjacent(relay.at[0])

    for gone, dst in absent:
        @pl.when(gone)
        def _(dst=dst):
            dst[...] = jnp.zeros(dst.shape, jnp.float32)
    zero = jnp.zeros((2, ring, cols), jnp.float32)
    for m in range(members):
        for end in (0, layers + 1):
            roots[m, end] = zero
            for c in range(2):
                ext[m, c, end] = zero
                pa[m, c, end] = zero
                pb[m, c, end] = zero
    cover_core = mask_v[...].astype(jnp.float32)
    for c in range(2):
        for z in range(layers):
            summed = u_v[0, c, z]
            for m in range(1, members):
                summed = summed + u_v[m, c, z]
            w_core[c, z] = cover_core * summed

    def arrive(k):
        for copy, to_ok, from_ok in flows[k]:
            pl.when(from_ok)(copy.wait_recv)
        _, _, group, groups = chunks[k]
        for g in range(group, group + groups):
            hx[g, 0:rows] = jnp.where(lane_x % 8 < 4, side_r[0, g], side_r[1, g])
            left = jnp.where(low8, corner_r[0, 0, g], corner_r[1, 0, g])
            right = jnp.where(low8, corner_r[0, 1, g], corner_r[1, 1, g])
            hx[g, rows:ring] = jnp.where(lane_x[0:8] % 8 < 4, left, right)

    def extended(k, p):
        pair, _, group, _ = chunks[k]
        i = pair + p // 2
        if p % 2 == 0:
            tail = jnp.where(low8, below_r[i], above_r[i])
        else:
            tail = pltpu.roll(jnp.where(low8, above_r[i], below_r[i]), 4, 0)
        core = jnp.concatenate([readers[k][p](), tail], axis=0)
        halo = pltpu.roll(hx[group + p // SLOTS], (-(8 * (p % SLOTS) + 4)) % cols, 1)
        return jnp.stack([core, halo])

    def assemble(m):
        arrive(m)
        base = places[m]
        for z in range(layers):
            for c in range(2):
                ext[m, c, z + 1] = extended(m, base + 2 * z + c)
        if m > 0:
            return
        bed = extended(0, 0)
        cover = extended(0, 1)
        row = iota((2, ring, cols), 1)
        position = (ix * rows + jnp.where(row < rows + HALO, row, row - ring)).astype(jnp.float32)
        thickness = 1.0 + 2.0 * position / (np_ * rows - 1)
        slope_x = (shift_i(bed, 1) - shift_i(bed, -1)) * 0.5
        slope_y = (shift_j(bed, 1) - shift_j(bed, -1)) * 0.5
        force[0] = -(cover * thickness * slope_x)
        force[1] = -(cover * thickness * slope_y)
        force[2] = cover
        force[3 + members] = 2.0 * cover
        for k in range(members):
            force[3 + k] = cover * extended(0, 2 + k)

    def roots_step(m, z):
        u, v = ext[m, 0, z + 1], ext[m, 1, z + 1]
        u_i = (shift_i(u, 1) - shift_i(u, -1)) * 0.5
        v_j = (shift_j(v, 1) - shift_j(v, -1)) * 0.5
        shear = ((shift_j(u, 1) - shift_j(u, -1)) + (shift_i(v, 1) - shift_i(v, -1))) * 0.5
        u_z = (ext[m, 0, z + 2] - ext[m, 0, z]) * 0.5
        v_z = (ext[m, 1, z + 2] - ext[m, 1, z]) * 0.5
        strain = (u_i * u_i + v_j * v_j + u_i * v_j + 0.25 * shear * shear
                  + 0.25 * (u_z * u_z + v_z * v_z))
        root = force[3 + members] * jnp.exp(jnp.log(strain + 0.1) * (-1.0 / 6.0))
        roots[m, z + 1] = root
        pa[m, 0, z + 1] = root * u
        pa[m, 1, z + 1] = root * v

    def image(m, c, z, field, p_ref):
        spread = spread_ij(spread_z(p_ref, (m, c), z), c)
        return tr[m, c, z] * field - roots[m, z + 1] * spread

    def residual_step(m, z, acc):
        near = spread_z(roots, (m,), z)
        diag = 1.0 - force[2]
        if z == 0:
            diag = diag + force[3 + m]
        for c in range(2):
            tr[m, c, z] = roots[m, z + 1] * spread_ij(near, c) + diag
            r = force[c] - image(m, c, z, force[2] * ext[m, c, z + 1], pa)
            r_ext[m, c, z] = r
            pb[m, c, z + 1] = roots[m, z + 1] * r
            core = r[0, 0:rows]
            r_core[m, c, z] = core
            acc = acc + core * core
        return acc

    def image_step(m, z, ra, aa):
        for c in range(2):
            r = r_ext[m, c, z]
            a = image(m, c, z, r, pb)
            a_ext[m, c, z] = a
            pa[m, c, z + 1] = roots[m, z + 1] * a
            core = a[0, 0:rows]
            a_core[m, c, z] = core
            ra = ra + r[0, 0:rows] * core
            aa = aa + core * core
        return ra, aa

    def second_step(m, z, ab):
        for c in range(2):
            a = a_ext[m, c, z]
            b = image(m, c, z, a, pa)
            ab = ab + a[0, 0:rows] * b[0, 0:rows]
        return ab

    peer = {"ens": lax.rem(ie + 1, ne)}

    def to_peer(i, src, dst):
        return pltpu.make_async_remote_copy(
            src_ref=src, dst_ref=dst, send_sem=peer_send.at[i], recv_sem=peer_recv.at[i],
            device_id=peer, device_id_type=mesh_id)

    peer_flows = [to_peer(0, w_core, w_peer)]
    for m in range(members):
        peer_flows.append(to_peer(2 * m + 1, r_core.at[m], r_peer.at[m]))
        peer_flows.append(to_peer(2 * m + 2, a_core.at[m], a_peer.at[m]))

    zero_core = jnp.zeros((rows, cols), jnp.float32)
    grams = []
    for m in range(members):
        assemble(m)
        for z in range(layers):
            roots_step(m, z)
        if m == 0:
            peer_flows[0].start()
            for k in range(1, rounds):
                pl.semaphore_wait(relay.at[k - 1], adjacent_count)
                signal_adjacent(relay.at[k])
        rr = ra = aa = ab = zero_core
        for z in range(layers):
            rr = residual_step(m, z, rr)
        for z in range(layers):
            ra, aa = image_step(m, z, ra, aa)
        peer_flows[2 * m + 1].start()
        for z in range(layers):
            ab = second_step(m, z, ab)
        peer_flows[2 * m + 2].start()
        grams.append((rr, ra, aa, ab))

    lane_1 = iota((1, cols), 1)
    mine = jnp.zeros((1, cols), jnp.float32)
    for m in range(members):
        for q, acc in enumerate(grams[m]):
            value = jnp.sum(jnp.sum(acc, axis=0, keepdims=True), axis=1, keepdims=True)
            mine = jnp.where(lane_1 == 4 * m + q, value, mine)
    gram_s[0] = mine

    if rounds > 0:
        pl.semaphore_wait(relay.at[rounds - 1], adjacent_count)

    def gram_copy(d):
        return pltpu.make_async_remote_copy(
            src_ref=gram_s, dst_ref=gram_r.at[pl.ds(d, 1)],
            send_sem=gram_send, recv_sem=gram_recv,
            device_id=group_target(d), device_id_type=pl.DeviceIdType.MESH)

    each_peer(lambda d: gram_copy(d).start())
    everything = pltpu.make_async_remote_copy(
        src_ref=gram_r.at[pl.ds(1, total - 1)], dst_ref=gram_r.at[pl.ds(1, total - 1)],
        send_sem=gram_send, recv_sem=gram_recv,
        device_id=group_target(1), device_id_type=pl.DeviceIdType.MESH)
    everything.wait_recv()

    half = np_ * nq
    own = mine
    if half > 1:
        own = own + jnp.sum(gram_r[1:half], axis=0)
    sums = [own] + [jnp.sum(gram_r[half * e:half * (e + 1)], axis=0) for e in range(1, ne)]
    steps = []
    for e in range(ne):
        for m in range(members):
            g_rr, g_ra, g_aa, g_ab = [
                jnp.sum(jnp.where(lane_1 == 4 * m + q, sums[e], 0.0), axis=1, keepdims=True)
                for q in range(4)
            ]
            first = g_rr / g_ra
            following = g_rr - 2.0 * first * g_ra + first * first * g_aa
            growth = 1.0 + following / g_rr
            curve = (growth * growth * g_ra - 2.0 * growth * first * g_aa
                     + first * first * g_ab)
            second = following / curve
            share = 1.0 / (members * ne)
            steps.append(((first + second * growth) * share, second * first * share))

    for flow in peer_flows:
        flow.wait_recv()
    share = 1.0 / (members * ne)

    def final_step(z, carry):
        for c in range(2):
            value = share * (w_core[c, z] + w_peer[c, z])
            for m in range(members):
                value = value + steps[m][0] * r_core[m, c, z] - steps[m][1] * a_core[m, c, z]
                one, two = steps[members + m]
                value = value + one * r_peer[m, c, z] - two * a_peer[m, c, z]
            out_ref[c, z] = value
        return carry

    lax.fori_loop(0, layers, final_step, 0)

    for chunk in flows:
        for copy, to_ok, from_ok in chunk:
            pl.when(to_ok)(copy.wait_send)
    for flow in peer_flows:
        flow.wait_send()
    everything.wait_send()


def body(sizes, u_prior, friction_rows, friction_table, bed_fixed, ice_mask):
    members, _, layers, rows, cols = u_prior.shape
    levels = friction_table.shape[0]
    total = sizes[0] * sizes[1] * sizes[2]
    ring = rows + 2 * HALO
    chunks, _ = chunk_places(members, layers)
    pairs = sum(chunk[1] for chunk in chunks)
    groups = sum(chunk[3] for chunk in chunks)
    f32 = jnp.float32
    any_space = pl.BlockSpec(memory_space=pl.ANY)
    vmem = lambda *shape: pltpu.VMEM(shape, f32)
    core = (members, 2, layers, rows, cols)
    wide = (2, ring, cols)
    return pl.pallas_call(
        functools.partial(kernel, sizes),
        out_shape=jax.ShapeDtypeStruct((2, layers, rows, cols), f32),
        in_specs=[any_space] * 5,
        out_specs=pl.BlockSpec(memory_space=pltpu.VMEM),
        scratch_shapes=[
            pltpu.SMEM((members,), jnp.int32), vmem(*core), vmem(levels, rows, cols),
            pltpu.VMEM((rows, cols), jnp.int32), pltpu.VMEM((rows, cols), jnp.int32),
            vmem(pairs, 8, cols), vmem(pairs, 8, cols), vmem(groups, rows, cols), vmem(groups, 8, cols),
            vmem(pairs, 8, cols), vmem(pairs, 8, cols), vmem(2, groups, rows, cols),
            vmem(2, 2, groups, 8, cols), vmem(groups, ring, cols),
            vmem(members, 2, layers + 2, *wide), vmem(members, layers + 2, *wide),
            vmem(members, 2, layers, *wide),
            vmem(members, 2, layers + 2, *wide), vmem(members, 2, layers + 2, *wide),
            vmem(members, 2, layers, *wide), vmem(members, 2, layers, *wide),
            vmem(4 + members, *wide),
            vmem(*core), vmem(*core), vmem(*core[1:]),
            vmem(*core), vmem(*core), vmem(*core[1:]),
            vmem(1, 1, cols), vmem(total, 1, cols),
            pltpu.SemaphoreType.REGULAR((max(sizes[0], sizes[1]),)),
            pltpu.SemaphoreType.DMA((5,)),
            pltpu.SemaphoreType.DMA((8 * members,)), pltpu.SemaphoreType.DMA((8 * members,)),
            pltpu.SemaphoreType.DMA((2 * members + 1,)), pltpu.SemaphoreType.DMA((2 * members + 1,)),
            pltpu.SemaphoreType.DMA, pltpu.SemaphoreType.DMA,
        ],
        compiler_params=pltpu.CompilerParams(
            collective_id=0, has_side_effects=True),
        name="picard",
    )(friction_rows, u_prior, friction_table, bed_fixed, ice_mask)


def solution(mesh):
    sizes = (mesh.shape["plane"], mesh.shape["planey"], mesh.shape["ens"])
    in_specs = (
        P(("group", "ens"), None, None, "plane", "planey"),
        P(("group", "ens")),
        P("group", "plane", "planey"),
        P("plane", "planey"),
        P("plane", "planey"),
    )
    out_specs = P("group", None, "plane", "planey")
    return jax.shard_map(functools.partial(body, sizes), mesh=mesh, in_specs=in_specs,
                         out_specs=out_specs, check_vma=False)
```
